128 devices in a mesh: rep: 1, dp: 128 (over x, y, z, core).
Axes of the slice: x: 4, y: 4, z: 4, core: 2. Of those that a mesh axis runs over, the one named last changes fastest.
Arguments:
- a: bfloat16 [128, 2, 4096, 1024], P(('rep', 'dp'))
- g: bfloat16 [128, 2, 4096, 3328], P(('rep', 'dp'))
Outputs:
- output: bfloat16 [2, 1024, 3328], P('rep')
All inputs are finite; a program needn't handle non-finite values.
Results may differ from the reference program's by a relative error of at most 0.012.
Values are sent between devices in bfloat16 or wider.
A program may use at most 1.5 GiB of HBM per device.

```python
import jax
import jax.numpy as jnp
from jax import lax

DEVICES = 128
MATRICES = 2
TOKENS = 4096
D = 1024
FF = 3328


def setup_inputs(seed: int = 0, part: int = 0) -> dict:
    ka, kg, ks = (jax.random.fold_in(k, part) for k in jax.random.split(jax.random.key(seed), 3))
    size = 2.0 ** jax.random.uniform(ks, (DEVICES, MATRICES, 1, 1), jnp.float32, -1.0, 1.0)
    a = jax.random.normal(ka, (DEVICES, MATRICES, TOKENS, D), jnp.float32)
    g = size * jax.random.normal(kg, (DEVICES, MATRICES, TOKENS, FF), jnp.float32) * (DEVICES * TOKENS) ** -0.5
    return {"a": a.astype(jnp.bfloat16), "g": g.astype(jnp.bfloat16)}


def reference(a, g):
    def take(so_far, one):
        term = jnp.einsum("ntd,ntf->ndf", *one, preferred_element_type=jnp.float32).astype(jnp.bfloat16)
        return so_far + term.astype(jnp.float32), None

    return lax.scan(take, jnp.zeros((MATRICES, D, FF), jnp.float32), (a, g))[0].astype(jnp.bfloat16)
```

```python
import jax
import jax.numpy as jnp
from jax import lax
from jax.experimental import pallas as pl
from jax.experimental.pallas import tpu as pltpu
from jax.sharding import PartitionSpec as P

MATRICES, TOKENS, D, FF = 2, 4096, 1024, 3328
WIDTH = 256
PER = FF // WIDTH
UNITS = MATRICES * PER
CHUNK = 512
CHUNKS = TOKENS // CHUNK
BF, F32 = jnp.bfloat16, jnp.float32
AT = (1, 3, 5, 7, 9, 10, 11, 12, 14, 16, 18)
DEPTH = AT[-1]


def kernel(
    a_ref, g_ref, out_ref,
    at_ref, araw, gbuf, tb, rp, r1, x1, s2, r2, x2, s3, r3,
    a_sem, g_sem, o_sem, pair_send, pair_recv, back_recv, send_sem, recv1, recv2, recv3, back1, back2, back3,
):
    me = lax.axis_index("dp")
    core = lax.rem(me, 2)
    partner = me + 1 - 2 * core
    cx, cy, cz = lax.div(me, 32), lax.rem(lax.div(me, 8), 4), lax.rem(lax.div(me, 2), 4)

    def to(device):
        return {"device_id": {"dp": device}, "device_id_type": pl.DeviceIdType.MESH}

    def remote(src, dst, ssem, rsem, device):
        return pltpu.make_async_remote_copy(src_ref=src, dst_ref=dst, send_sem=ssem, recv_sem=rsem, **to(device))

    def wait_for(ref, sem):
        pltpu.make_async_copy(ref, ref, sem).wait()

    def along(m, stride, off):
        return me + (lax.rem(m + off + 4, 4) - m) * stride

    barrier = pltpu.get_barrier_semaphore()
    pl.semaphore_signal(barrier, inc=1, **to(partner))
    for m, stride in ((cx, 32), (cy, 8), (cz, 2)):
        for off in (1, 2, 3):
            pl.semaphore_signal(barrier, inc=1, **to(along(m, stride, off)))

    def a_copy(n, k, slot):
        return pltpu.make_async_copy(a_ref.at[0, n, pl.ds(k * CHUNK, CHUNK)], araw.at[slot], a_sem.at[slot])

    def g_copy(u, slot):
        n = lax.div(u, PER)
        col = pl.multiple_of((u - n * PER) * WIDTH, WIDTH)
        return pltpu.make_async_copy(g_ref.at[0, n, :, pl.ds(col, WIDTH)], gbuf.at[slot], g_sem.at[slot])

    a_copy(0, 0, 0).start()
    a_copy(0, 1, 1).start()
    g_copy(0, 0).start()

    def turn(n, k, slot):
        at_ref[n, :, pl.ds(pl.multiple_of(k * CHUNK, CHUNK), CHUNK)] = araw[slot].T

    def first(k, _):
        slot = lax.rem(k, 2)
        a_copy(0, k, slot).wait()
        turn(0, k, slot)

        @pl.when(k < CHUNKS - 2)
        def _():
            a_copy(0, k + 2, slot).start()

        return 0

    lax.fori_loop(0, CHUNKS, first, 0)
    a_copy(1, 0, 0).start()
    a_copy(1, 1, 1).start()
    pl.semaphore_wait(barrier, 10)

    def place(u):
        k = lax.rem(u, 3)
        e0, e1, e2 = lax.div((1 - k) * (2 - k), 2), k * (2 - k), lax.div(k * (k - 1), 2)
        dims = ((cx, 32), (cy, 8), (cz, 2))
        res = []
        for p in range(3):
            (ma, sa), (mb, sb), (mc, sc) = dims[p], dims[(p + 1) % 3], dims[(p + 2) % 3]
            res.append((e0 * ma + e1 * mb + e2 * mc, e0 * sa + e1 * sb + e2 * sc))
        return res

    def way(u):
        return 1 - 2 * lax.rem(lax.div(u, 3), 2)

    def term(u, rows):
        return tb[u, core, rows].astype(F32)

    def events(t):
        def at(stage):
            return t - AT[stage]

        def on(stage):
            def wrap(f):
                u = at(stage)
                pl.when((u >= 0) & (u < UNITS))(lambda: f(u))

            return wrap

        @on(0)
        def _(u):
            (m, stride), _, _ = place(u)
            s = way(u)
            wait_for(rp.at[u], pair_recv.at[u])
            wait_for(rp.at[u], pair_send.at[u])
            for i, (q, off) in enumerate(((m + 2, s), (m - s, -s))):
                rows = pl.ds(lax.rem(q + 4, 4) * 16, 16)
                rp[u, rows] = (term(u, rows) + rp[u, rows].astype(F32)).astype(BF)
                remote(rp.at[u, rows], r1.at[u, i], send_sem.at[u], recv1.at[u, i], along(m, stride, off)).start()

        @on(1)
        def _(u):
            (m, stride), _, _ = place(u)
            s = way(u)
            wait_for(r1.at[u, 0], recv1.at[u, 0])
            rows = pl.ds(lax.rem(m + s + 4, 4) * 16, 16)
            rp[u, rows] = (term(u, rows) + rp[u, rows].astype(F32) + r1[u, 0].astype(F32)).astype(BF)
            remote(rp.at[u, rows], r1.at[u, 2], send_sem.at[u], recv1.at[u, 2], along(m, stride, s)).start()

        @on(2)
        def _(u):
            (m1, _), (m, stride), _ = place(u)
            wait_for(r1.at[u, 1], recv1.at[u, 1])
            wait_for(r1.at[u, 2], recv1.at[u, 2])
            rows = pl.ds(m1 * 16, 16)
            x1[u] = (term(u, rows) + rp[u, rows].astype(F32)) + (r1[u, 1].astype(F32) + r1[u, 2].astype(F32))
            for i in range(3):
                off = i + 1
                s2[u, i] = x1[u, pl.ds(lax.rem(m + off, 4) * 4, 4)].astype(BF)
                remote(s2.at[u, i], r2.at[u, i], send_sem.at[u], recv2.at[u, i], along(m, stride, off)).start()

        @on(3)
        def _(u):
            _, (m2, _), (m, stride) = place(u)
            for i in range(3):
                wait_for(r2.at[u, i], recv2.at[u, i])
            x2[u] = (x1[u, pl.ds(m2 * 4, 4)] + r2[u, 0].astype(F32)) + (r2[u, 1].astype(F32) + r2[u, 2].astype(F32))
            for i in range(3):
                off = i + 1
                s3[u, i] = x2[u, pl.ds(lax.rem(m + off, 4), 1)].astype(BF)
                remote(s3.at[u, i], r3.at[u, i], send_sem.at[u], recv3.at[u, i], along(m, stride, off)).start()

        @on(4)
        def _(u):
            (m1, _), (m2, _), (m, stride) = place(u)
            for i in range(3):
                wait_for(r3.at[u, i], recv3.at[u, i])
            rows = pl.ds(m1 * 16 + m2 * 4 + m, 1)
            tb[u, core, rows] = (
                (x2[u, pl.ds(m, 1)] + r3[u, 0].astype(F32)) + (r3[u, 1].astype(F32) + r3[u, 2].astype(F32))
            ).astype(BF)
            for i in range(3):
                block = tb.at[u, core, rows]
                remote(block, block, send_sem.at[u], back3.at[u, i], along(m, stride, i + 1)).start()

        @on(5)
        def _(u):
            (m1, _), (m, stride), _ = place(u)
            for i in range(3):
                wait_for(tb.at[u, 0, pl.ds(0, 1)], back3.at[u, i])
            block = tb.at[u, core, pl.ds(m1 * 16 + m * 4, 4)]
            for i in range(3):
                remote(block, block, send_sem.at[u], back2.at[u, i], along(m, stride, i + 1)).start()

        @on(6)
        def _(u):
            (m, stride), _, _ = place(u)
            s = way(u)
            for i in range(3):
                wait_for(tb.at[u, 0, pl.ds(0, 4)], back2.at[u, i])
            block = tb.at[u, core, pl.ds(m * 16, 16)]
            for i, off in enumerate((s, -s)):
                remote(block, block, send_sem.at[u], back1.at[u, i], along(m, stride, off)).start()

        @on(7)
        def _(u):
            (m, stride), _, _ = place(u)
            s = way(u)
            wait_for(tb.at[u, 0, pl.ds(0, 16)], back1.at[u, 0])
            block = tb.at[u, core, pl.ds(lax.rem(m - s + 4, 4) * 16, 16)]
            remote(block, block, send_sem.at[u], back1.at[u, 2], along(m, stride, s)).start()

        @on(8)
        def _(u):
            wait_for(tb.at[u, 0, pl.ds(0, 16)], back1.at[u, 1])
            wait_for(tb.at[u, 0, pl.ds(0, 16)], back1.at[u, 2])
            block = tb.at[u, core]
            remote(block, block, send_sem.at[u], back_recv.at[u], partner).start()

        @on(9)
        def _(u):
            wait_for(tb.at[u, 0], back_recv.at[u])
            n = lax.div(u, PER)
            for h in range(2):
                col = pl.multiple_of((u - n * PER) * WIDTH + h * 128, 128)
                pltpu.make_async_copy(tb.at[u, h], out_ref.at[n, :, :, pl.ds(col, 128)], o_sem.at[u]).start()

        @on(10)
        def _(u):
            wait_for(tb.at[u], o_sem.at[u])
            wait_for(gbuf.at[0, pl.ds(0, 190 * 8)], send_sem.at[u])

    def loop(t, _):
        n = lax.div(t, PER)
        slot = lax.rem(t, 2)
        g_copy(t, slot).wait()

        @pl.when(t < UNITS - 1)
        def _():
            g_copy(t + 1, 1 - slot).start()

        acc = lax.dot_general(
            at_ref[n], gbuf[slot], (((1,), (0,)), ((), ())), preferred_element_type=F32
        ).astype(BF)
        for h in range(2):
            tb[t, h] = acc[:, h * 128 : (h + 1) * 128].reshape(64, 16, 128)
        remote(tb.at[t, 1 - core], rp.at[t], pair_send.at[t], pair_recv.at[t], partner).start()

        @pl.when(t < CHUNKS)
        def _():
            a_copy(1, t, slot).wait()
            turn(1, t, slot)

            @pl.when(t < CHUNKS - 2)
            def _():
                a_copy(1, t + 2, slot).start()

        events(t)
        return 0

    lax.fori_loop(0, UNITS, loop, 0)
    lax.fori_loop(UNITS, UNITS + DEPTH, lambda t, _: (events(t), 0)[1], 0)


def solution(mesh):
    dma, tile = pltpu.SemaphoreType.DMA, (16, 128)

    def body(a, g):
        out = pl.pallas_call(
            kernel,
            out_shape=jax.ShapeDtypeStruct((MATRICES, D // 16, 16, FF), BF),
            in_specs=[pl.BlockSpec(memory_space=pl.ANY)] * 2,
            out_specs=pl.BlockSpec(memory_space=pl.ANY),
            scratch_shapes=[
                pltpu.VMEM((MATRICES, D, TOKENS), BF),
                pltpu.VMEM((2, CHUNK, D), BF),
                pltpu.VMEM((2, TOKENS, WIDTH), BF),
                pltpu.VMEM((UNITS, 2, 64, *tile), BF),
                pltpu.VMEM((UNITS, 64, *tile), BF),
                pltpu.VMEM((UNITS, 3, 16, *tile), BF),
                pltpu.VMEM((UNITS, 16, *tile), F32),
                pltpu.VMEM((UNITS, 3, 4, *tile), BF),
                pltpu.VMEM((UNITS, 3, 4, *tile), BF),
                pltpu.VMEM((UNITS, 4, *tile), F32),
                pltpu.VMEM((UNITS, 3, 1, *tile), BF),
                pltpu.VMEM((UNITS, 3, 1, *tile), BF),
                dma((2,)),
                dma((2,)),
                dma((UNITS,)),
                dma((UNITS,)),
                dma((UNITS,)),
                dma((UNITS,)),
                dma((UNITS,)),
                *[dma((UNITS, 3))] * 6,
            ],
            compiler_params=pltpu.CompilerParams(
                collective_id=0, has_side_effects=True, vmem_limit_bytes=67043328
            ),
            cost_estimate=pl.CostEstimate(
                flops=2 * MATRICES * TOKENS * D * FF, bytes_accessed=100_000_000, transcendentals=0
            ),
        )(a, g)
        return out.reshape(MATRICES, D, FF)

    return jax.shard_map(
        body,
        mesh=mesh,
        in_specs=(P(("rep", "dp")), P(("rep", "dp"))),
        out_specs=P("rep"),
        check_vma=False,
    )
```

```python
import jax
import jax.numpy as jnp
from jax import lax
from jax.experimental import pallas as pl
from jax.experimental.pallas import tpu as pltpu
from jax.sharding import PartitionSpec as P

MATRICES, TOKENS, D, FF = 2, 4096, 1024, 3328
WIDTH = 256
PER = FF // WIDTH
UNITS = MATRICES * PER
CHUNK = 512
CHUNKS = TOKENS // CHUNK
BF, F32 = jnp.bfloat16, jnp.float32
DIRECT = 20
RELAYED = (1, 3, 5, 7, 9, 11, 13, 15, 17, 18)
STRAIGHT = (1, None, 3, 5, 7, 9, 11, None, 13, 14)
LAST = UNITS - 1 + STRAIGHT[-1]


def kernel(
    a_ref, g_ref, tb,
    at_ref, araw, gbuf, total, rp, r1, x1, s2, r2, x2, s3, r3,
    a_sem, g_sem, pair_send, pair_recv, back_recv, send_sem, far1, recv1, recv2, recv3, over1, back1, back2, back3,
):
    me = lax.axis_index("dp")
    core = lax.rem(me, 2)
    partner = me + 1 - 2 * core
    cx, cy, cz = lax.div(me, 32), lax.rem(lax.div(me, 8), 4), lax.rem(lax.div(me, 2), 4)

    def to(device):
        return {"device_id": {"dp": device}, "device_id_type": pl.DeviceIdType.MESH}

    def remote(src, dst, ssem, rsem, device):
        return pltpu.make_async_remote_copy(src_ref=src, dst_ref=dst, send_sem=ssem, recv_sem=rsem, **to(device))

    def wait_for(ref, sem):
        pltpu.make_async_copy(ref, ref, sem).wait()

    def along(m, stride, off):
        return me + (lax.rem(m + off + 4, 4) - m) * stride

    barrier = pltpu.get_barrier_semaphore()
    pl.semaphore_signal(barrier, inc=1, **to(partner))
    for m, stride in ((cx, 32), (cy, 8), (cz, 2)):
        for off in (1, 2, 3):
            pl.semaphore_signal(barrier, inc=1, **to(along(m, stride, off)))

    def a_copy(n, k, slot):
        return pltpu.make_async_copy(a_ref.at[0, n, pl.ds(k * CHUNK, CHUNK)], araw.at[slot], a_sem.at[slot])

    def g_copy(u, slot):
        n = lax.div(u, PER)
        col = pl.multiple_of((u - n * PER) * WIDTH, WIDTH)
        return pltpu.make_async_copy(g_ref.at[0, n, :, pl.ds(col, WIDTH)], gbuf.at[slot], g_sem.at[slot])

    a_copy(0, 0, 0).start()
    a_copy(0, 1, 1).start()
    g_copy(0, 0).start()

    def turned(slot):
        return araw[slot].T

    def piece(k):
        return pl.ds(pl.multiple_of(k * CHUNK, CHUNK), CHUNK)

    def product(left, right):
        return lax.dot_general(left, right, (((1,), (0,)), ((), ())), preferred_element_type=F32)

    g_copy(0, 0).wait()
    g_copy(1, 1).start()
    total[...] = jnp.zeros_like(total)

    def first(k, _):
        slot = lax.rem(k, 2)
        a_copy(0, k, slot).wait()
        block = turned(slot)
        at_ref[0, :, piece(k)] = block
        total[...] += product(block, gbuf[0, piece(k)])
        a_copy(lax.div(k, CHUNKS - 2), lax.rem(k + 2, CHUNKS), slot).start()
        return 0

    lax.fori_loop(0, CHUNKS, first, 0)
    pl.semaphore_wait(barrier, 10)

    def keep(t, acc):
        acc = acc.astype(BF)
        for h in range(2):
            tb[t, h] = acc[:, h * 128 : (h + 1) * 128].reshape(64, 16, 128)
        remote(tb.at[t, 1 - core], rp.at[t], pair_send.at[t], pair_recv.at[t], partner).start()

    keep(0, total[...])

    def place(u):
        k = lax.rem(u, 3)
        e0, e1, e2 = lax.div((1 - k) * (2 - k), 2), k * (2 - k), lax.div(k * (k - 1), 2)
        dims = ((cx, 32), (cy, 8), (cz, 2))
        res = []
        for p in range(3):
            (ma, sa), (mb, sb), (mc, sc) = dims[p], dims[(p + 1) % 3], dims[(p + 2) % 3]
            res.append((e0 * ma + e1 * mb + e2 * mc, e0 * sa + e1 * sb + e2 * sc))
        return res

    def way(u):
        return 1 - 2 * lax.rem(lax.div(u, 3), 2)

    def term(u, rows):
        return tb[u, core, rows].astype(F32)

    def events(t, straight, lo=0, hi=99):
        stages = STRAIGHT if straight else RELAYED
        begin, end = (DIRECT, UNITS) if straight else (0, DIRECT)

        def on(stage):
            def wrap(f):
                if stages[stage] is None or not lo <= stages[stage] <= hi:
                    return
                u = t - stages[stage]
                pl.when((u >= begin) & (u < end))(lambda: f(u))

            return wrap

        @on(0)
        def _(u):
            (m, stride), _, _ = place(u)
            s = way(u)
            wait_for(rp.at[u], pair_recv.at[u])
            wait_for(rp.at[u], pair_send.at[u])

            def send(i, q, off, sem):
                rows = pl.ds(lax.rem(q + 4, 4) * 16, 16)
                rp[u, rows] = (term(u, rows) + rp[u, rows].astype(F32)).astype(BF)
                remote(rp.at[u, rows], r1.at[u, i], send_sem.at[u], sem.at[u], along(m, stride, off)).start()

            if straight:
                send(0, m + 2, 2, recv1)
                send(1, m - s, -s, recv1)
                send(2, m + s, s, recv1)
            else:
                send(0, m + 2, s, far1)
                send(1, m - s, -s, recv1)

        @on(1)
        def _(u):
            (m, stride), _, _ = place(u)
            s = way(u)
            wait_for(r1.at[u, 0], far1.at[u])
            rows = pl.ds(lax.rem(m + s + 4, 4) * 16, 16)
            rp[u, rows] = (term(u, rows) + rp[u, rows].astype(F32) + r1[u, 0].astype(F32)).astype(BF)
            remote(rp.at[u, rows], r1.at[u, 2], send_sem.at[u], recv1.at[u], along(m, stride, s)).start()

        @on(2)
        def _(u):
            (m1, _), (m, stride), _ = place(u)
            rows = pl.ds(m1 * 16, 16)
            came = r1.at[u] if straight else r1.at[u, pl.ds(1, 2)]
            wait_for(came, recv1.at[u])
            got = r1[u, 1].astype(F32) + r1[u, 2].astype(F32)
            if straight:
                got += r1[u, 0].astype(F32)
            x1[u] = (term(u, rows) + rp[u, rows].astype(F32)) + got
            for i in range(3):
                off = i + 1
                s2[u, i] = x1[u, pl.ds(lax.rem(m + off, 4) * 4, 4)].astype(BF)
                remote(s2.at[u, i], r2.at[u, i], send_sem.at[u], recv2.at[u], along(m, stride, off)).start()

        @on(3)
        def _(u):
            _, (m2, _), (m, stride) = place(u)
            wait_for(r2.at[u], recv2.at[u])
            x2[u] = (x1[u, pl.ds(m2 * 4, 4)] + r2[u, 0].astype(F32)) + (r2[u, 1].astype(F32) + r2[u, 2].astype(F32))
            for i in range(3):
                off = i + 1
                s3[u, i] = x2[u, pl.ds(lax.rem(m + off, 4), 1)].astype(BF)
                remote(s3.at[u, i], r3.at[u, i], send_sem.at[u], recv3.at[u], along(m, stride, off)).start()

        @on(4)
        def _(u):
            (m1, _), (m2, _), (m, stride) = place(u)
            wait_for(r3.at[u], recv3.at[u])
            rows = pl.ds(m1 * 16 + m2 * 4 + m, 1)
            tb[u, core, rows] = (
                (x2[u, pl.ds(m, 1)] + r3[u, 0].astype(F32)) + (r3[u, 1].astype(F32) + r3[u, 2].astype(F32))
            ).astype(BF)
            for i in range(3):
                block = tb.at[u, core, rows]
                remote(block, block, send_sem.at[u], back3.at[u], along(m, stride, i + 1)).start()

        @on(5)
        def _(u):
            (m1, _), (m, stride), _ = place(u)
            wait_for(tb.at[u, 0, pl.ds(0, 3)], back3.at[u])
            block = tb.at[u, core, pl.ds(m1 * 16 + m * 4, 4)]
            for i in range(3):
                remote(block, block, send_sem.at[u], back2.at[u], along(m, stride, i + 1)).start()

        @on(6)
        def _(u):
            (m, stride), _, _ = place(u)
            s = way(u)
            wait_for(tb.at[u, 0, pl.ds(0, 12)], back2.at[u])
            block = tb.at[u, core, pl.ds(m * 16, 16)]

            def send(off, sem):
                remote(block, block, send_sem.at[u], sem.at[u], along(m, stride, off)).start()

            if straight:
                send(2, back1)
                send(1, back1)
                send(3, back1)
            else:
                send(s, over1)
                send(-s, back1)

        @on(7)
        def _(u):
            (m, stride), _, _ = place(u)
            s = way(u)
            wait_for(tb.at[u, 0, pl.ds(0, 16)], over1.at[u])
            block = tb.at[u, core, pl.ds(lax.rem(m - s + 4, 4) * 16, 16)]
            remote(block, block, send_sem.at[u], back1.at[u], along(m, stride, s)).start()

        @on(8)
        def _(u):
            wait_for(tb.at[u, 0, pl.ds(0, 48 if straight else 32)], back1.at[u])
            block = tb.at[u, core]
            remote(block, block, send_sem.at[u], back_recv.at[u], partner).start()

        @on(9)
        def _(u):
            wait_for(tb.at[u, 0], back_recv.at[u])
            wait_for(gbuf.at[0, pl.ds(0, 190 * 8)], send_sem.at[u])

    def loop(t, turning, lo, hi):
        slot = lax.rem(t, 2)
        g_copy(t, slot).wait()

        @pl.when(t < UNITS - 1)
        def _():
            g_copy(t + 1, 1 - slot).start()

        if turning:
            k = t - 1
            half = lax.rem(k, 2)
            a_copy(1, k, half).wait()
            acc = product(at_ref[0], gbuf[slot])
            at_ref[1, :, piece(k)] = turned(half)
            keep(t, acc)

            @pl.when(k < CHUNKS - 2)
            def _():
                a_copy(1, k + 2, half).start()

        else:
            keep(t, product(at_ref[lax.div(t, PER)], gbuf[slot]))
        events(t, False, lo, hi)
        if hi > CHUNKS:
            pl.when(t > DIRECT)(lambda: events(t, True, 0, UNITS - 1 - DIRECT))
        return 0

    def tail(t, _):
        events(t, False, UNITS - DIRECT + 1, 99)
        events(t, True)
        return 0

    lax.fori_loop(1, CHUNKS + 1, lambda t, _: loop(t, True, 0, CHUNKS), 0)
    lax.fori_loop(CHUNKS + 1, UNITS, lambda t, _: loop(t, False, 0, 99), 0)
    lax.fori_loop(UNITS, LAST + 1, tail, 0)


def write(tb, out_ref, sem):
    copies = []
    for n in range(MATRICES):
        for j in range(PER):
            for h in range(2):
                block = out_ref.at[n, :, :, pl.ds(j * WIDTH + h * 128, 128)]
                copies.append(pltpu.make_async_copy(tb.at[n * PER + j, h], block, sem.at[n, j, h]))
    for copy in copies:
        copy.start()
    for copy in copies:
        copy.wait()


def solution(mesh):
    dma, tile = pltpu.SemaphoreType.DMA, (16, 128)

    def body(a, g):
        out = pl.pallas_call(
            kernel,
            out_shape=pltpu.VMEM((UNITS, 2, 64, *tile), BF),
            in_specs=[pl.BlockSpec(memory_space=pl.ANY)] * 2,
            out_specs=pl.BlockSpec(memory_space=pltpu.VMEM),
            scratch_shapes=[
                pltpu.VMEM((MATRICES, D, TOKENS), BF),
                pltpu.VMEM((2, CHUNK, D), BF),
                pltpu.VMEM((2, TOKENS, WIDTH), BF),
                pltpu.VMEM((D, WIDTH), F32),
                pltpu.VMEM((UNITS, 64, *tile), BF),
                pltpu.VMEM((UNITS, 3, 16, *tile), BF),
                pltpu.VMEM((UNITS, 16, *tile), F32),
                pltpu.VMEM((UNITS, 3, 4, *tile), BF),
                pltpu.VMEM((UNITS, 3, 4, *tile), BF),
                pltpu.VMEM((UNITS, 4, *tile), F32),
                pltpu.VMEM((UNITS, 3, 1, *tile), BF),
                pltpu.VMEM((UNITS, 3, 1, *tile), BF),
                dma((2,)),
                dma((2,)),
                *[dma((UNITS,))] * 12,
            ],
            compiler_params=pltpu.CompilerParams(
                collective_id=0, has_side_effects=True, vmem_limit_bytes=50 << 20
            ),
            cost_estimate=pl.CostEstimate(
                flops=2 * MATRICES * TOKENS * D * FF, bytes_accessed=100_000_000, transcendentals=0
            ),
        )(a, g)
        out = pl.pallas_call(
            write,
            out_shape=jax.ShapeDtypeStruct((MATRICES, D // 16, 16, FF), BF),
            in_specs=[pl.BlockSpec(memory_space=pltpu.VMEM)],
            out_specs=pl.BlockSpec(memory_space=pl.ANY),
            scratch_shapes=[dma((MATRICES, PER, 2))],
            compiler_params=pltpu.CompilerParams(vmem_limit_bytes=1 << 20),
        )(pltpu.with_memory_space_constraint(out, pltpu.VMEM))
        return out.reshape(MATRICES, D, FF)

    return jax.shard_map(
        body,
        mesh=mesh,
        in_specs=(P(("rep", "dp")), P(("rep", "dp"))),
        out_specs=P("rep"),
        check_vma=False,
    )
```

```python
import jax
import jax.numpy as jnp
from jax import lax
from jax.experimental import pallas as pl
from jax.experimental.pallas import tpu as pltpu
from jax.sharding import PartitionSpec as P

MATRICES, TOKENS, D, FF = 2, 4096, 1024, 3328
WIDTH = 256
PER = FF // WIDTH
UNITS = MATRICES * PER
CHUNK = 512
CHUNKS = TOKENS // CHUNK
BF, F32 = jnp.bfloat16, jnp.float32
DIRECT = 22
RELAYED = (1, 3, 5, 7, 9, 11, 13, 15, 17, 18)
STRAIGHT = (1, None, 3, 5, 7, 9, 11, None, 13, 14)
LAST = max(UNITS - 1 + STRAIGHT[-1], DIRECT - 1 + RELAYED[-1])


def kernel(
    a_ref, g_ref, tb,
    at_ref, araw, gbuf, total, rp, r1, x1, s2, r2, x2, s3, r3,
    a_sem, g_sem, pair_send, pair_recv, back_recv, send_sem, far1, recv1, recv2, recv3, over1, back1, back2, back3,
):
    me = lax.axis_index("dp")
    core = lax.rem(me, 2)
    partner = me + 1 - 2 * core
    cx, cy, cz = lax.div(me, 32), lax.rem(lax.div(me, 8), 4), lax.rem(lax.div(me, 2), 4)

    def to(device):
        return {"device_id": {"dp": device}, "device_id_type": pl.DeviceIdType.MESH}

    def remote(src, dst, ssem, rsem, device):
        return pltpu.make_async_remote_copy(src_ref=src, dst_ref=dst, send_sem=ssem, recv_sem=rsem, **to(device))

    def wait_for(ref, sem):
        pltpu.make_async_copy(ref, ref, sem).wait()

    def along(m, stride, off):
        return me + (lax.rem(m + off + 4, 4) - m) * stride

    barrier = pltpu.get_barrier_semaphore()
    pl.semaphore_signal(barrier, inc=1, **to(partner))
    for m, stride in ((cx, 32), (cy, 8), (cz, 2)):
        for off in (1, 2, 3):
            pl.semaphore_signal(barrier, inc=1, **to(along(m, stride, off)))

    def a_copy(n, k, slot):
        return pltpu.make_async_copy(a_ref.at[0, n, pl.ds(k * CHUNK, CHUNK)], araw.at[slot], a_sem.at[slot])

    def g_copy(u, slot):
        n = lax.div(u, PER)
        col = pl.multiple_of((u - n * PER) * WIDTH, WIDTH)
        return pltpu.make_async_copy(g_ref.at[0, n, :, pl.ds(col, WIDTH)], gbuf.at[slot], g_sem.at[slot])

    a_copy(0, 0, 0).start()
    a_copy(0, 1, 1).start()
    g_copy(0, 0).start()

    def turned(slot):
        return araw[slot].T

    def piece(k):
        return pl.ds(pl.multiple_of(k * CHUNK, CHUNK), CHUNK)

    def product(left, right):
        return lax.dot_general(left, right, (((1,), (0,)), ((), ())), preferred_element_type=F32)

    g_copy(0, 0).wait()
    g_copy(1, 1).start()
    total[...] = jnp.zeros_like(total)

    def first(k, _):
        slot = lax.rem(k, 2)
        a_copy(0, k, slot).wait()
        block = turned(slot)
        at_ref[0, :, piece(k)] = block
        total[...] += product(block, gbuf[0, piece(k)])
        a_copy(lax.div(k, CHUNKS - 2), lax.rem(k + 2, CHUNKS), slot).start()
        return 0

    lax.fori_loop(0, CHUNKS, first, 0)
    pl.semaphore_wait(barrier, 10)

    def keep(t, acc):
        acc = acc.astype(BF)
        for h in range(2):
            tb[t, h] = acc[:, h * 128 : (h + 1) * 128].reshape(64, 16, 128)
        remote(tb.at[t, 1 - core], rp.at[t], pair_send.at[t], pair_recv.at[t], partner).start()

    keep(0, total[...])

    def place(u):
        k = lax.rem(u + core, 3)
        e0, e1, e2 = lax.div((1 - k) * (2 - k), 2), k * (2 - k), lax.div(k * (k - 1), 2)
        dims = ((cx, 32), (cy, 8), (cz, 2))
        res = []
        for p in range(3):
            (ma, sa), (mb, sb), (mc, sc) = dims[p], dims[(p + 1) % 3], dims[(p + 2) % 3]
            res.append((e0 * ma + e1 * mb + e2 * mc, e0 * sa + e1 * sb + e2 * sc))
        return res

    def way(u):
        return 1 - 2 * lax.rem(lax.div(u, 3), 2)

    def term(u, rows):
        return tb[u, core, rows].astype(F32)

    def events(t, straight, lo=0, hi=99):
        stages = STRAIGHT if straight else RELAYED
        begin, end = (DIRECT, UNITS) if straight else (0, DIRECT)

        def on(stage):
            def wrap(f):
                if stages[stage] is None or not lo <= stages[stage] <= hi:
                    return
                u = t - stages[stage]
                pl.when((u >= begin) & (u < end))(lambda: f(u))

            return wrap

        @on(0)
        def _(u):
            (m, stride), _, _ = place(u)
            s = way(u)
            wait_for(rp.at[u], pair_recv.at[u])
            wait_for(rp.at[u], pair_send.at[u])

            def send(i, q, off, sem):
                rows = pl.ds(lax.rem(q + 4, 4) * 16, 16)
                rp[u, rows] = (term(u, rows) + rp[u, rows].astype(F32)).astype(BF)
                remote(rp.at[u, rows], r1.at[u, i], send_sem.at[u], sem.at[u], along(m, stride, off)).start()

            if straight:
                send(0, m + 2, 2, recv1)
                send(1, m - s, -s, recv1)
                send(2, m + s, s, recv1)
            else:
                send(0, m + 2, s, far1)
                send(1, m - s, -s, recv1)

        @on(1)
        def _(u):
            (m, stride), _, _ = place(u)
            s = way(u)
            wait_for(r1.at[u, 0], far1.at[u])
            rows = pl.ds(lax.rem(m + s + 4, 4) * 16, 16)
            rp[u, rows] = (term(u, rows) + rp[u, rows].astype(F32) + r1[u, 0].astype(F32)).astype(BF)
            remote(rp.at[u, rows], r1.at[u, 2], send_sem.at[u], recv1.at[u], along(m, stride, s)).start()

        @on(2)
        def _(u):
            (m1, _), (m, stride), _ = place(u)
            rows = pl.ds(m1 * 16, 16)
            came = r1.at[u] if straight else r1.at[u, pl.ds(1, 2)]
            wait_for(came, recv1.at[u])
            got = r1[u, 1].astype(F32) + r1[u, 2].astype(F32)
            if straight:
                got += r1[u, 0].astype(F32)
            x1[u] = (term(u, rows) + rp[u, rows].astype(F32)) + got
            for i in range(3):
                off = i + 1
                s2[u, i] = x1[u, pl.ds(lax.rem(m + off, 4) * 4, 4)].astype(BF)
                remote(s2.at[u, i], r2.at[u, i], send_sem.at[u], recv2.at[u], along(m, stride, off)).start()

        @on(3)
        def _(u):
            _, (m2, _), (m, stride) = place(u)
            wait_for(r2.at[u], recv2.at[u])
            x2[u] = (x1[u, pl.ds(m2 * 4, 4)] + r2[u, 0].astype(F32)) + (r2[u, 1].astype(F32) + r2[u, 2].astype(F32))
            for i in range(3):
                off = i + 1
                s3[u, i] = x2[u, pl.ds(lax.rem(m + off, 4), 1)].astype(BF)
                remote(s3.at[u, i], r3.at[u, i], send_sem.at[u], recv3.at[u], along(m, stride, off)).start()

        @on(4)
        def _(u):
            (m1, _), (m2, _), (m, stride) = place(u)
            wait_for(r3.at[u], recv3.at[u])
            rows = pl.ds(m1 * 16 + m2 * 4 + m, 1)
            tb[u, core, rows] = (
                (x2[u, pl.ds(m, 1)] + r3[u, 0].astype(F32)) + (r3[u, 1].astype(F32) + r3[u, 2].astype(F32))
            ).astype(BF)
            for i in range(3):
                block = tb.at[u, core, rows]
                remote(block, block, send_sem.at[u], back3.at[u], along(m, stride, i + 1)).start()

        @on(5)
        def _(u):
            (m1, _), (m, stride), _ = place(u)
            wait_for(tb.at[u, 0, pl.ds(0, 3)], back3.at[u])
            block = tb.at[u, core, pl.ds(m1 * 16 + m * 4, 4)]
            for i in range(3):
                remote(block, block, send_sem.at[u], back2.at[u], along(m, stride, i + 1)).start()

        @on(6)
        def _(u):
            (m, stride), _, _ = place(u)
            s = way(u)
            wait_for(tb.at[u, 0, pl.ds(0, 12)], back2.at[u])
            block = tb.at[u, core, pl.ds(m * 16, 16)]

            def send(off, sem):
                remote(block, block, send_sem.at[u], sem.at[u], along(m, stride, off)).start()

            if straight:
                send(2, back1)
                send(1, back1)
                send(3, back1)
            else:
                send(s, over1)
                send(-s, back1)

        @on(7)
        def _(u):
            (m, stride), _, _ = place(u)
            s = way(u)
            wait_for(tb.at[u, 0, pl.ds(0, 16)], over1.at[u])
            block = tb.at[u, core, pl.ds(lax.rem(m - s + 4, 4) * 16, 16)]
            remote(block, block, send_sem.at[u], back1.at[u], along(m, stride, s)).start()

        @on(8)
        def _(u):
            wait_for(tb.at[u, 0, pl.ds(0, 48 if straight else 32)], back1.at[u])
            block = tb.at[u, core]
            remote(block, block, send_sem.at[u], back_recv.at[u], partner).start()

        @on(9)
        def _(u):
            wait_for(tb.at[u, 0], back_recv.at[u])
            wait_for(gbuf.at[0, pl.ds(0, 190 * 8)], send_sem.at[u])

    def loop(t, turning, lo, hi):
        slot = lax.rem(t, 2)
        g_copy(t, slot).wait()

        @pl.when(t < UNITS - 1)
        def _():
            g_copy(t + 1, 1 - slot).start()

        if turning:
            k = t - 1
            half = lax.rem(k, 2)
            a_copy(1, k, half).wait()
            acc = product(at_ref[0], gbuf[slot])
            at_ref[1, :, piece(k)] = turned(half)
            keep(t, acc)

            @pl.when(k < CHUNKS - 2)
            def _():
                a_copy(1, k + 2, half).start()

        else:
            keep(t, product(at_ref[lax.div(t, PER)], gbuf[slot]))
        events(t, False, lo, hi)
        if hi > CHUNKS:
            pl.when(t > DIRECT)(lambda: events(t, True, 0, UNITS - 1 - DIRECT))
        return 0

    def tail(t, _):
        events(t, True)
        events(t, False, UNITS - DIRECT + 1, 99)
        return 0

    lax.fori_loop(1, CHUNKS + 1, lambda t, _: loop(t, True, 0, CHUNKS), 0)
    lax.fori_loop(CHUNKS + 1, UNITS, lambda t, _: loop(t, False, 0, 99), 0)
    lax.fori_loop(UNITS, LAST + 1, tail, 0)


def write(tb, out_ref, sem):
    copies = []
    for n in range(MATRICES):
        for j in range(PER):
            for h in range(2):
                block = out_ref.at[n, :, :, pl.ds(j * WIDTH + h * 128, 128)]
                copies.append(pltpu.make_async_copy(tb.at[n * PER + j, h], block, sem.at[n, j, h]))
    for copy in copies:
        copy.start()
    for copy in copies:
        copy.wait()


def solution(mesh):
    dma, tile = pltpu.SemaphoreType.DMA, (16, 128)

    def body(a, g):
        out = pl.pallas_call(
            kernel,
            out_shape=pltpu.VMEM((UNITS, 2, 64, *tile), BF),
            in_specs=[pl.BlockSpec(memory_space=pl.ANY)] * 2,
            out_specs=pl.BlockSpec(memory_space=pltpu.VMEM),
            scratch_shapes=[
                pltpu.VMEM((MATRICES, D, TOKENS), BF),
                pltpu.VMEM((2, CHUNK, D), BF),
                pltpu.VMEM((2, TOKENS, WIDTH), BF),
                pltpu.VMEM((D, WIDTH), F32),
                pltpu.VMEM((UNITS, 64, *tile), BF),
                pltpu.VMEM((UNITS, 3, 16, *tile), BF),
                pltpu.VMEM((UNITS, 16, *tile), F32),
                pltpu.VMEM((UNITS, 3, 4, *tile), BF),
                pltpu.VMEM((UNITS, 3, 4, *tile), BF),
                pltpu.VMEM((UNITS, 4, *tile), F32),
                pltpu.VMEM((UNITS, 3, 1, *tile), BF),
                pltpu.VMEM((UNITS, 3, 1, *tile), BF),
                dma((2,)),
                dma((2,)),
                *[dma((UNITS,))] * 12,
            ],
            compiler_params=pltpu.CompilerParams(
                collective_id=0, has_side_effects=True, vmem_limit_bytes=50 << 20
            ),
            cost_estimate=pl.CostEstimate(
                flops=2 * MATRICES * TOKENS * D * FF, bytes_accessed=100_000_000, transcendentals=0
            ),
        )(a, g)
        out = pl.pallas_call(
            write,
            out_shape=jax.ShapeDtypeStruct((MATRICES, D // 16, 16, FF), BF),
            in_specs=[pl.BlockSpec(memory_space=pltpu.VMEM)],
            out_specs=pl.BlockSpec(memory_space=pl.ANY),
            scratch_shapes=[dma((MATRICES, PER, 2))],
            compiler_params=pltpu.CompilerParams(vmem_limit_bytes=1 << 20),
        )(pltpu.with_memory_space_constraint(out, pltpu.VMEM))
        return out.reshape(MATRICES, D, FF)

    return jax.shard_map(
        body,
        mesh=mesh,
        in_specs=(P(("rep", "dp")), P(("rep", "dp"))),
        out_specs=P("rep"),
        check_vma=False,
    )
```
